32 devices in a mesh: expert: 16 (over z, y, core), dp: 2 (over x).
Axes of the slice: x: 2, y: 2, z: 4, core: 2. Of those that a mesh axis runs over, the one named last changes fastest.
Arguments:
- tokens: bfloat16 [4096, 4096], P(('expert', 'dp')), may hold values from -6 to 6
- route: int32 [4096, 2], P(('expert', 'dp')), may hold values from 0 to 31, all different within a row; in each aligned block of 128 rows (0 to 127, 128 to 255, ...) at most 24 rows name the same one
- gate_output_gradient: bfloat16 [4096, 2, 1536], P(('expert', 'dp')), may hold values from -0.4375 to 0.4375
- frozen_gate_weight: bfloat16 [32, 4096, 1536], P('expert', 'dp'), may hold values from -0.09375 to 0.09375
- adapter_first: bfloat16 [32, 4096, 16], P('expert'), may hold values from -0.09375 to 0.09375
- adapter_second: bfloat16 [32, 16, 1536], P('expert'), may hold values from -0.15625 to 0.15625
Outputs:
- grad_a: float32 [32, 4096, 16], P('expert')
- grad_b: float32 [32, 16, 1536], P('expert')
The draws below stay inside these ranges and needn't reach their ends.
Inputs may be any that keep to these rules, and one draw needn't show every extreme that they name: `route`: each row names 2 different experts. Within each device's aligned block of 128 rows no expert is named more than 24 times.
All inputs are finite; a program needn't handle non-finite values.
Results may differ from the reference program's by a relative error of at most 0.0043.
Values may be sent and summed in bfloat16 or wider, within the bound.
A program may use at most 128 MiB of HBM per device.

```python
import math
import jax
import jax.numpy as jnp
import numpy as np
from jax import lax

MODEL_WIDTH = 4096
GATE_HIDDEN = 1536
ADAPTER_RANK = 16
TOP = 2
TOK_DEV = 128
EXPERT_TOTAL = 32
CAP = 24
TOKENS = 4096


def levels(own_key, shape, pieces, low, high):
    gain, own = 1.0, jax.random.fold_in(own_key, 6)
    for dim, parts in pieces:
        heights = jnp.exp(jax.random.uniform(jax.random.fold_in(own, dim), (parts,), jnp.float32, low / len(pieces), high / len(pieces)))
        gain = gain * jnp.repeat(heights, shape[dim] // parts).reshape([-1 if axis == dim else 1 for axis in range(len(shape))])
    return gain


def assign_block(stream_key, own, number, rows, amount, top, bound, lean):
    order = jax.random.permutation(stream_key, amount)
    heavy_load, common = load_shares(amount, rows * top, bound, lean, True), load_shares(amount, rows * top, bound, lean, False)
    places = jnp.arange(amount)

    def named(sizes, rotation):
        used = int((sizes > 0).sum())
        fixed = max(1, used // 4)
        shifted = fixed + (places - fixed + rotation * (used - fixed)) % max(1, amount - fixed)
        return jnp.zeros((amount,), jnp.int32).at[order[jnp.where(places < fixed, places, shifted)]].set(jnp.asarray(sizes, jnp.int32))

    sizes = jnp.where(number % 4 == 0, named(heavy_load, number // 4), named(common, number - number // 4 - 1))
    mixed = jax.random.permutation(jax.random.fold_in(own, 3), amount)
    source_of, receiver = mixed[0:amount // 2 * 2:2], mixed[1:amount // 2 * 2:2]
    slack = jnp.minimum(sizes[source_of] - 1, bound - sizes[receiver]) // 2
    slack = jnp.where((source_of == order[0]) | (receiver == order[0]) | (sizes[receiver] == 0), 0, jnp.maximum(slack, 0))
    shifted = jax.random.randint(jax.random.fold_in(own, 4), (amount // 2,), 0, 1 << 20) % (slack + 1)
    sizes = sizes.at[source_of].add(-shifted).at[receiver].add(shifted)
    items = jnp.searchsorted(jnp.cumsum(sizes), jnp.arange(rows * top), side="right").astype(jnp.int32)
    table = items.reshape(top, rows).T
    table = table[jax.random.permutation(jax.random.fold_in(own, 1), rows)]
    rotation = jax.random.randint(jax.random.fold_in(own, 2), (rows, 1), 0, top)
    return jnp.take_along_axis(table, (jnp.arange(top)[None, :] + rotation) % top, axis=1)


def load_shares(amount, total, limit, lean, full):
    portions = [(1 << 20) // math.isqrt(standing ** lean) + 1 for standing in range(1, amount + 1)]
    largest = limit if full else min(limit, max(-(-total // amount), total * portions[0] // sum(portions)))
    least = 1 if total - largest >= amount - 1 else 0
    given, rest = [largest] + [least] * (amount - 1), total - largest - least * (amount - 1)
    while rest > 0:
        movable = [i for i in range(1, amount) if given[i] < largest] or [i for i in range(1, amount) if given[i] < limit]
        pool, budget = sum([portions[i] for i in movable]), rest
        for i in movable:
            extra = min(limit - given[i], max(1, budget * portions[i] // pool), rest)
            given[i] = given[i] + extra
            rest = rest - extra
    return np.array(given)


def gaussian(rng, shape, deviation, most, split=(), kind=jnp.bfloat16):
    gain = levels(rng, shape, split, -0.22, 0.18) if split else 1.0
    drawn = jax.random.normal(rng, shape, jnp.float32) * deviation * gain
    return jnp.minimum(jnp.maximum(drawn, -most), most).astype(kind)


def setup_inputs(seed: int = 0) -> dict:
    splits = jax.random.split(jax.random.key(seed), 7)
    tokens = gaussian(splits[0], (TOKENS, MODEL_WIDTH), 1.0, 6.0, ((0, 32),))
    route_keys = jax.random.split(jax.random.fold_in(splits[1], 1), TOKENS // TOK_DEV)
    route_turns = jax.random.permutation(jax.random.fold_in(splits[1], 3), TOKENS // TOK_DEV)
    route = jax.vmap(lambda own, number: assign_block(jax.random.fold_in(splits[1], 2), own, number, TOK_DEV, EXPERT_TOTAL, TOP, CAP, 2))(route_keys, route_turns).reshape((TOKENS, TOP))
    gate_output_gradient = gaussian(splits[2], (TOKENS, TOP, GATE_HIDDEN), 0.03, 0.4375, ((0, 32),))
    frozen_gate_weight = gaussian(splits[3], (EXPERT_TOTAL, MODEL_WIDTH, GATE_HIDDEN), MODEL_WIDTH ** -0.5, 0.09375, ((0, 16), (1, 2)))
    adapter_first = gaussian(splits[4], (EXPERT_TOTAL, MODEL_WIDTH, ADAPTER_RANK), MODEL_WIDTH ** -0.5, 0.09375, ((0, 16),))
    adapter_second = gaussian(splits[5], (EXPERT_TOTAL, ADAPTER_RANK, GATE_HIDDEN), GATE_HIDDEN ** -0.5, 0.15625, ((0, 16),))
    return dict(tokens=tokens, route=route, gate_output_gradient=gate_output_gradient, frozen_gate_weight=frozen_gate_weight, adapter_first=adapter_first, adapter_second=adapter_second)


ADAPTER_SCALE = 2.0


def silu_slope(gate_preactivation):
    squash = jax.nn.sigmoid(gate_preactivation)
    return squash * (1.0 + gate_preactivation * (1.0 - squash))


def reference(tokens, route, gate_output_gradient, frozen_gate_weight, adapter_first, adapter_second):
    group_rows = 512
    slot_count = TOKENS * TOP
    flat_route = route.reshape(slot_count).astype(jnp.int32)
    order = jnp.argsort(flat_route, stable=True).astype(jnp.int32)
    labels = jnp.arange(EXPERT_TOTAL, dtype=jnp.int32)
    counts = jnp.sum((flat_route[:, None] == labels[None, :]).astype(jnp.int32), axis=0)
    starts = jnp.cumsum(counts) - counts
    padded = (counts + group_rows - 1) // group_rows * group_rows
    pad_starts = jnp.cumsum(padded) - padded
    block_count = slot_count // group_rows + EXPERT_TOTAL
    flat_grad = gate_output_gradient.reshape(slot_count, GATE_HIDDEN)

    def one_block(carry, block_index):
        down_gradient, up_gradient = carry
        first = block_index * group_rows
        expert_index = (jnp.sum((pad_starts <= first).astype(jnp.int32)) - 1).astype(jnp.int32)
        within = first + jnp.arange(group_rows, dtype=jnp.int32) - pad_starts[expert_index]
        valid = within < counts[expert_index]
        source = order[jnp.clip(starts[expert_index] + within, 0, slot_count - 1)]
        input_rows = tokens[source // TOP]
        rows_g = jnp.where(valid[:, None], flat_grad[source], jnp.zeros((), flat_grad.dtype))
        weight = frozen_gate_weight[expert_index]
        first_adapter_factor = adapter_first[expert_index]
        second_adapter_factor = adapter_second[expert_index]
        frozen_output = jnp.dot(input_rows, weight, preferred_element_type=jnp.float32)
        rank_reduced_output = jnp.dot(input_rows, first_adapter_factor, preferred_element_type=jnp.float32).astype(jnp.bfloat16)
        gate_preactivation = frozen_output + ADAPTER_SCALE * jnp.dot(rank_reduced_output, second_adapter_factor, preferred_element_type=jnp.float32)
        activation_slope = (rows_g.astype(jnp.float32) * silu_slope(gate_preactivation)).astype(jnp.bfloat16)
        up_portion = ADAPTER_SCALE * jnp.dot(rank_reduced_output.T, activation_slope, preferred_element_type=jnp.float32)
        rank_backward = jnp.dot(activation_slope, second_adapter_factor.T, preferred_element_type=jnp.float32).astype(jnp.bfloat16)
        down_portion = ADAPTER_SCALE * jnp.dot(input_rows.T, rank_backward, preferred_element_type=jnp.float32)
        down_gradient = down_gradient.at[expert_index].add(down_portion)
        up_gradient = up_gradient.at[expert_index].add(up_portion)
        return (down_gradient, up_gradient), None

    initial = (jnp.zeros((EXPERT_TOTAL, MODEL_WIDTH, ADAPTER_RANK), jnp.float32), jnp.zeros((EXPERT_TOTAL, ADAPTER_RANK, GATE_HIDDEN), jnp.float32))
    (grad_a, grad_b), _ = lax.scan(one_block, initial, jnp.arange(block_count, dtype=jnp.int32))
    return grad_a, grad_b
```

```python
import jax
import jax.numpy as jnp
from jax import lax
from jax.sharding import PartitionSpec as P

ADAPTER_SCALE = 2.0
RING = 4
F32 = jnp.float32


def silu_slope(gate_preactivation):
    squash = jax.nn.sigmoid(gate_preactivation)
    return squash * (1.0 + gate_preactivation * (1.0 - squash))


def dot(spec, a, b):
    return jnp.einsum(spec, a, b, preferred_element_type=F32)


def slot_codes(route, experts, capacity):
    tok_rows, top_count = route.shape
    flat_route = route.reshape(tok_rows * top_count)
    labels = jnp.arange(experts, dtype=jnp.int32)
    one_hot = (flat_route[:, None] == labels[None, :]).astype(jnp.int32)
    ranks = jnp.sum((jnp.cumsum(one_hot, axis=0) - one_hot) * one_hot, axis=1)
    return (flat_route * capacity + ranks).reshape(tok_rows, top_count)


def local(tokens, route, gate_output_gradient, frozen_gate_weight, adapter_first, adapter_second):
    experts_here, part, hidden = frozen_gate_weight.shape
    columns, halves = lax.axis_size("expert"), lax.axis_size("dp")
    experts = experts_here * columns
    tok_rows, width = tokens.shape
    top_count = route.shape[1]
    capacity = 3 * tok_rows * top_count // experts
    hidden_part = hidden // halves
    ring = RING if columns % RING == 0 else 1
    inner = columns // ring
    column, me = lax.axis_index("expert"), lax.axis_index("dp")
    outer_at, inner_at = column // inner, column % inner

    codes = slot_codes(route, experts, capacity)
    all_codes = lax.all_gather(codes, ("expert", "dp")).reshape(
        columns, halves, tok_rows, top_count
    )

    def piece(target):
        parts = [lax.dynamic_slice_in_dim(tokens, target * part, part, 1)]
        for k in range(top_count):
            parts.append(
                lax.dynamic_slice_in_dim(
                    gate_output_gradient[:, k], target * hidden_part, hidden_part, 1
                )
            )
        return jnp.concatenate(parts, axis=1)

    def dp_shift(value, k):
        return lax.ppermute(value, "dp", [(i, (i + k) % halves) for i in range(halves)])

    def dp_sum(value):
        total = value
        for k in range(1, halves):
            total = total + dp_shift(jnp.roll(value, k, axis=1), k)
        return total

    streams = [(piece(me)[None], [0])]
    if halves > 1:
        others = [dp_shift(piece((me + k) % halves), k) for k in range(1, halves)]
        streams.append((jnp.stack(others), list(range(1, halves))))

    around = [(i, (i + inner) % columns) for i in range(columns)]
    first_part = lax.dynamic_slice_in_dim(adapter_first, me * part, part, 1)
    second_part = lax.dynamic_slice_in_dim(adapter_second, me * hidden_part, hidden_part, 2)
    group = experts_here * capacity
    places = (
        (outer_at * inner + (inner_at + jnp.arange(inner, dtype=jnp.int32)) % inner)[:, None]
        * group
        + jnp.arange(group, dtype=jnp.int32)[None, :]
    ).reshape(inner * group)

    grad_a, grad_b = 0.0, 0.0
    blocks = [stream[0] for stream in streams]
    for step in range(ring):
        source = (outer_at + ring - step) % ring * inner + inner_at
        step_codes = lax.dynamic_index_in_dim(all_codes, source, 0, keepdims=False)
        following, step_rows = [], []
        for (_, shifts), block in zip(streams, blocks):
            if step < ring - 1:
                following.append(lax.ppermute(block, "expert", around))
            count = len(shifts)
            own_codes = jnp.stack(
                [
                    lax.dynamic_index_in_dim(step_codes, (me + halves - k) % halves, 0, keepdims=False)
                    for k in shifts
                ]
            )
            picks = [
                (own_codes[:, None, :, k] == places[None, :, None]).astype(jnp.bfloat16)
                for k in range(top_count)
            ]
            packed_x = dot("mrt,mtw->mrw", sum(picks[1:], picks[0]), block[:, :, :part])
            packed_g = sum(
                dot(
                    "mrt,mtw->mrw",
                    picks[k],
                    block[:, :, part + k * hidden_part : part + (k + 1) * hidden_part],
                )
                for k in range(top_count)
            )
            packed = jnp.concatenate(
                [packed_x.astype(jnp.bfloat16), packed_g.astype(jnp.bfloat16)], axis=2
            ).reshape(count, inner, group, part + hidden_part)
            arrived = [packed[:, 0]]
            for j in range(1, inner):
                pairs = [
                    (o * inner + i, o * inner + (i + j) % inner)
                    for o in range(ring)
                    for i in range(inner)
                ]
                arrived.append(lax.ppermute(packed[:, j], "expert", pairs))
            step_rows.append(
                jnp.stack(arrived, 1).reshape(count, inner, experts_here, capacity, -1)
            )
        rows = jnp.concatenate(step_rows, axis=0).transpose(2, 0, 1, 3, 4)
        rows = rows.reshape(experts_here, halves, inner * capacity, -1)
        rows_x, rows_g = rows[..., :part], rows[..., part:]
        partial = dot("ednw,ewf->ednf", rows_x, frozen_gate_weight)
        low = dp_sum(dot("ednw,ewr->ednr", rows_x, first_part)).astype(jnp.bfloat16)

        def take(target):
            return lax.dynamic_slice_in_dim(partial, target * hidden_part, hidden_part, 3)

        preact = take(me) + ADAPTER_SCALE * dot("ednr,erf->ednf", low, second_part)
        for k in range(1, halves):
            sent = jnp.roll(take((me + k) % halves).astype(jnp.bfloat16), k, axis=1)
            preact = preact + dp_shift(sent, k).astype(F32)
        slope = (rows_g.astype(F32) * silu_slope(preact)).astype(jnp.bfloat16)
        back = dp_sum(dot("ednf,erf->ednr", slope, second_part)).astype(jnp.bfloat16)
        grad_b = grad_b + dot("ednr,ednf->erf", low, slope)
        grad_a = grad_a + dot("ednr,ednw->erw", back, rows_x)
        blocks = following

    joined = ADAPTER_SCALE * jnp.concatenate([grad_a, grad_b], axis=2)
    whole = lax.all_gather(joined, "dp")
    whole_a = whole[:, :, :, :part].transpose(1, 0, 3, 2).reshape(experts_here, width, -1)
    whole_b = whole[:, :, :, part:].transpose(1, 2, 0, 3).reshape(experts_here, -1, hidden)
    return (whole_a, whole_b)


def solution(mesh):
    return jax.shard_map(
        local,
        mesh=mesh,
        in_specs=(
            P(("expert", "dp"), None),
            P(("expert", "dp"), None),
            P(("expert", "dp"), None, None),
            P("expert", "dp", None),
            P("expert", None, None),
            P("expert", None, None),
        ),
        out_specs=(P("expert", None, None), P("expert", None, None)),
        check_vma=False,
    )
```
